32 devices in a mesh: chain: 16 (over z, x, core), tok: 2 (over y).
Axes of the slice: x: 2, y: 2, z: 4, core: 2. Of those that a mesh axis runs over, the one named last changes fastest.
Arguments:
- queries: bfloat16 [65536, 128], P(('chain', 'tok')), may hold values from -6 to 6
- keys: bfloat16 [65536, 128], P(('chain', 'tok')), may hold values from -6 to 6
- values: bfloat16 [65536, 128], P(('chain', 'tok')), may hold values from -6 to 6
Outputs:
- attended: bfloat16 [65536, 128], P(('chain', 'tok'))
The draws below stay inside these ranges and needn't reach their ends.
All inputs are finite; a program needn't handle non-finite values.
Results may differ from the reference program's by a relative error of at most 0.0058.
Values may be sent and summed in bfloat16 or wider, within the bound.
A program may use at most 64 MiB of HBM per device.

```python
import math
import jax
import jax.numpy as jnp
import numpy as np
from jax import lax

HD = 64
HEADS = 2
F = 2080
GROUP = 4096
TOKENS = 65536
N_CHAIN = 16


def levels(key, shape, pieces, low, largest):
    factor_of, own = 1.0, jax.random.fold_in(key, 6)
    for dim, parts in pieces:
        draws = jnp.exp(jax.random.uniform(jax.random.fold_in(own, dim), (parts,), jnp.float32, low / len(pieces), largest / len(pieces)))
        factor_of = factor_of * jnp.repeat(draws, shape[dim] // parts).reshape([-1 if axis == dim else 1 for axis in range(len(shape))])
    return factor_of


def normal_values(own_key, dims, scale, reach, pieces=(), held_as=jnp.bfloat16):
    array = scale * jax.random.normal(own_key, dims, jnp.float32)
    if pieces:
        array = array * levels(own_key, dims, pieces, -0.22, 0.18)
    return jnp.clip(array, -reach, reach).astype(held_as)


def setup_inputs(seed: int = 0) -> dict:
    streams_of = jax.random.split(jax.random.key(seed), 4)
    return {
        "queries": normal_values(streams_of[0], (TOKENS, HEADS * HD), 1.0, 6.0, ((0, 32),)),
        "keys": normal_values(streams_of[1], (TOKENS, HEADS * HD), 1.0, 6.0, ((0, 32),)),
        "values": normal_values(streams_of[2], (TOKENS, HEADS * HD), 1.0, 6.0, ((0, 32),)),
    }


def tables(width):
    first, second = np.triu_indices(width)
    places = np.arange(width)[:, None]
    first_pick = (places == first[None, :]).astype(np.float32)
    second_pick = (places == second[None, :]).astype(np.float32)
    scaling = np.where(first < second, math.sqrt(2.0), 1.0).astype(np.float32)
    return (jnp.asarray(first_pick), jnp.asarray(second_pick), jnp.asarray(scaling))

def expand(vectors, first_pick, second_pick, scaling):
    wide = vectors.astype(jnp.float32)
    left = jnp.dot(wide, first_pick, precision=lax.Precision.HIGHEST)
    right = jnp.dot(wide, second_pick, precision=lax.Precision.HIGHEST)
    rounded = (left * right * scaling[None, :]).astype(jnp.bfloat16)
    return lax.optimization_barrier(rounded).astype(jnp.float32)

def reference(queries, keys, values):
    first_pick, second_pick, scaling = tables(HD)
    shaped_q = jnp.transpose(queries.reshape(N_CHAIN, GROUP, HEADS, HD), (0, 2, 1, 3))
    shaped_k = jnp.transpose(keys.reshape(N_CHAIN, GROUP, HEADS, HD), (0, 2, 1, 3))
    shaped_v = jnp.transpose(values.reshape(N_CHAIN, GROUP, HEADS, HD), (0, 2, 1, 3))

    def head_state(pair):
        key_rows, value_rows = pair
        feats = expand(key_rows, first_pick, second_pick, scaling)
        return jnp.dot(feats.T, value_rows.astype(jnp.float32), precision=lax.Precision.HIGHEST)

    def head_read(pair):
        query_rows, state = pair
        feats = expand(query_rows, first_pick, second_pick, scaling)
        return jnp.dot(feats, state.astype(jnp.float32), precision=lax.Precision.HIGHEST)

    def step(prefix, inputs):
        index, query_group, key_group, value_group = inputs
        total = lax.map(head_state, (key_group, value_group))
        inclusive = prefix + total
        rounded = inclusive.astype(jnp.bfloat16)
        read = lax.map(head_read, (query_group, rounded))
        count = (index + 1).astype(jnp.float32) * GROUP
        result = (read / (HD * jnp.sqrt(count))).astype(jnp.bfloat16)
        return (inclusive, result)
    start = jnp.zeros((HEADS, F, HD), jnp.float32)
    order = jnp.arange(N_CHAIN, dtype=jnp.int32)
    _, outputs = lax.scan(step, start, (order, shaped_q, shaped_k, shaped_v))
    return jnp.transpose(outputs, (0, 2, 1, 3)).reshape(TOKENS, HEADS * HD)
```

```python
import functools
import math

import jax
import jax.numpy as jnp
from jax import lax
from jax.experimental import pallas as pl
from jax.experimental.pallas import tpu as pltpu
from jax.sharding import PartitionSpec as P

HD = 64
HEADS = 2
WIDE = HEADS * HD
HALF = HD // 2
BLOCKS = HD // 4 + 1
LANES, DEEP = 128, 256
MESH = pl.DeviceIdType.MESH
F32, BF16 = jnp.float32, jnp.bfloat16


def layout(n_chain, n_tok):
    inner = 1 << ((n_chain.bit_length() - 1) // 2)
    plane = inner * n_tok
    row_parts = min(8, plane)
    blk_parts = plane // row_parts
    units = -(-BLOCKS // blk_parts)
    count = min(3, units)
    cuts = [-(-units * c // count) for c in range(count + 1)]
    return inner, plane, row_parts, blk_parts, units, cuts


def pairs(low, high):
    return [tuple(range(b, min(b + 2, high))) for b in range(low, high, 2)]


def kernel(n_chain, n_tok, q_ref, k_ref, v_ref, o_ref, xs, zs, qf, tot, got, plane_sum,
           far_got, inc_send, inc, out_t, rs_send, rs_recv, z_send, z_recv, ag_send, ag_recv):
    inner, plane, row_parts, blk_parts, units, cuts = layout(n_chain, n_tok)
    outer = n_chain // inner
    rows = WIDE // row_parts
    tokens = q_ref.shape[0]
    tiles = tokens // LANES
    chain, tok = lax.axis_index("chain"), lax.axis_index("tok")
    z, me = chain // inner, (chain % inner) * n_tok + tok

    def in_plane(k):
        peer = (me + k) % plane
        return peer, (z * inner + peer // n_tok, peer % n_tok)

    def along(k):
        return (((z + k) % outer) * inner + chain % inner, tok)

    barrier = pltpu.get_barrier_semaphore()
    for k in range(1, plane):
        pl.semaphore_signal(barrier, inc=1, device_id=in_plane(k)[1], device_id_type=MESH)
    for k in range(1, outer):
        pl.semaphore_signal(barrier, inc=1, device_id=along(k), device_id_type=MESH)

    root2 = math.sqrt(2.0)

    def prepare(ref):
        @pl.loop(0, tiles)
        def _(t):
            x = ref[pl.ds(pl.multiple_of(t * LANES, LANES), LANES), :].astype(F32).T
            for h in range(HEADS):
                own = x[h * HD:(h + 1) * HD]
                xs[h, t] = own
                wide = own * root2
                zs[h, t, pl.ds(0, HD), :] = wide
                zs[h, t, pl.ds(HD, HALF), :] = wide[:HALF]

    def feats(h, t, d):
        x = xs[h, t]
        if d == 0:
            other = x
        elif d == HALF:
            other = jnp.concatenate([x[HALF:], x[:HALF]], axis=0)
        else:
            other = zs[h, t, pl.ds(d, HD), :]
        return (x * other).astype(BF16)

    def joined(parts, axis=1):
        return parts[0] if len(parts) == 1 else jnp.concatenate(parts, axis=axis)

    def dists(b):
        return [d for d in (2 * b, 2 * b + 1) if d <= HALF]

    def blocks_of(c):
        return cuts[c] * blk_parts, cuts[c + 1] * blk_parts

    def state(c):
        low, high = blocks_of(c)
        real = min(high, BLOCKS)
        for group in pairs(low, real):
            ds = [d for b in group for d in dists(b)]
            parts = []
            for h in range(HEADS):
                part = None
                for k in range(tokens // DEEP):
                    lhs = joined([joined([feats(h, t, d) for d in ds], axis=0)
                                  for t in range(k * DEEP // LANES, (k + 1) * DEEP // LANES)])
                    more = jnp.dot(lhs, v_ref[pl.ds(k * DEEP, DEEP), :], preferred_element_type=F32)
                    part = more if part is None else part + more
                parts.append(part)
            left = lax.broadcasted_iota(jnp.int32, parts[0].shape, 1) < HD
            both = jnp.where(left, parts[0], parts[1])
            short = len(group) * WIDE - both.shape[0]
            if short:
                both = jnp.concatenate([both, jnp.zeros((short, WIDE), F32)], axis=0)
            for i, b in enumerate(group):
                tot[b] = both[i * WIDE:(i + 1) * WIDE].T.astype(BF16)
        if high > max(low, real):
            first = max(low, real)
            tot[pl.ds(first, high - first)] = jnp.zeros((high - first, WIDE, WIDE), BF16)

    def spot(c, who):
        low, _ = blocks_of(c)
        size = cuts[c + 1] - cuts[c]
        row = pl.multiple_of((who % row_parts) * rows, rows)
        return pl.ds(low + (who // row_parts) * size, size), pl.ds(row, rows)

    def span(c):
        return pl.ds(cuts[c], cuts[c + 1] - cuts[c])

    started = []

    def scatter(c):
        for k in range(1, plane):
            peer, device = in_plane(k)
            blk, row = spot(c, peer)
            copy = pltpu.make_async_remote_copy(
                src_ref=tot.at[blk, row, :], dst_ref=got.at[k, span(c)],
                send_sem=rs_send.at[c, k], recv_sem=rs_recv.at[c, k],
                device_id=device, device_id_type=MESH)
            copy.start()
            started.append(copy)
            rs_copies[c].append(copy)
        blk, row = spot(c, me)
        got[0, span(c)] = tot[blk, row, :]

    def piece(c, source):
        return got[(me + plane - source) % plane, span(c)].astype(F32)

    def spread(c):
        for copy in rs_copies[c]:
            copy.wait_recv()
        total = piece(c, 0)
        for source in range(1, plane):
            total = total + piece(c, source)
        plane_sum[span(c)] = total.astype(BF16)
        for k in range(1, outer):
            copy = pltpu.make_async_remote_copy(
                src_ref=plane_sum.at[span(c)], dst_ref=far_got.at[k, span(c)],
                send_sem=z_send.at[c, k], recv_sem=z_recv.at[c, k],
                device_id=along(k), device_id_type=MESH)
            copy.start()
            started.append(copy)
            z_copies[c].append(copy)

    def gather(c):
        running = jnp.zeros((cuts[c + 1] - cuts[c], rows, WIDE), F32)
        for k in range(1, outer):
            z_copies[c][k - 1].wait_recv()
            running = running + jnp.where(k <= z, far_got[k, span(c)].astype(F32), 0.0)
        for g in range(inner):
            for y in range(n_tok):
                running = running + piece(c, g * n_tok + y)
            inc_send[g, span(c)] = running.astype(BF16)
        blk, row = spot(c, me)
        for k in range(1, plane):
            peer, device = in_plane(k)
            copy = pltpu.make_async_remote_copy(
                src_ref=inc_send.at[peer // n_tok, span(c)], dst_ref=inc.at[blk, row, :],
                send_sem=ag_send.at[c, k], recv_sem=ag_recv.at[c, k],
                device_id=device, device_id_type=MESH)
            copy.start()
            started.append(copy)
            ag_copies[c].append(copy)
        inc[blk, row, :] = inc_send[chain % inner, span(c)]

    def expand_queries(c):
        low, high = blocks_of(c)

        @pl.loop(0, tiles)
        def _(t):
            at = pl.ds(pl.multiple_of(t * LANES, LANES), LANES)
            for b in range(low, min(high, BLOCKS)):
                for d in dists(b):
                    for h in range(HEADS):
                        qf[h, pl.ds(d * HD, HD), at] = feats(h, t, d)

    def read(c, first, last):
        for copy in ag_copies[c]:
            copy.wait_recv()
        low, high = blocks_of(c)
        groups = pairs(low, min(high, BLOCKS))
        count = (chain + 1).astype(F32) * (tokens * n_tok)
        factor = 1.0 / (HD * jnp.sqrt(jnp.full((LANES, WIDE), count, F32)))
        for k in range(tokens // DEEP):
            at = pl.ds(k * DEEP, DEEP)
            sums = []
            for h in range(HEADS):
                row = pl.ds(h * HD, HD)
                part = None if first else out_t[row, at]
                for group in groups:
                    depth = sum(len(dists(b)) for b in group) * HD
                    state_t = joined([inc[b, row, :] for b in group])[:, :depth]
                    more = jnp.dot(state_t, qf[h, pl.ds(group[0] * WIDE, depth), at],
                                   preferred_element_type=F32)
                    part = more if part is None else part + more
                if last:
                    sums.append(part)
                else:
                    out_t[row, at] = part
            if last:
                whole = jnp.concatenate(sums, axis=0)
                for i in range(DEEP // LANES):
                    o_ref[pl.ds(k * DEEP + i * LANES, LANES), :] = (
                        whole[:, i * LANES:(i + 1) * LANES].T * factor).astype(BF16)

    n = len(cuts) - 1
    rs_copies, z_copies, ag_copies = ([[] for _ in range(n)] for _ in range(3))

    prepare(k_ref)

    for c in range(n):
        state(c)
        if c == 0:
            pl.semaphore_wait(barrier, plane - 1 + outer - 1)
        scatter(c)
        if c >= 1:
            spread(c - 1)
    prepare(q_ref)
    for c in range(n):
        expand_queries(c)
        if c == 0:
            spread(n - 1)
        gather(c)
    for c in range(n):
        read(c, c == 0, c == n - 1)
    for copy in started:
        copy.wait_send()


def on_device(n_chain, n_tok, queries, keys, values):
    inner, plane, row_parts, blk_parts, units, cuts = layout(n_chain, n_tok)
    outer, n = n_chain // inner, len(cuts) - 1
    rows, tokens = WIDE // row_parts, queries.shape[0]
    blocks = units * blk_parts
    sems = pltpu.SemaphoreType.DMA
    return pl.pallas_call(
        functools.partial(kernel, n_chain, n_tok),
        out_shape=jax.ShapeDtypeStruct((tokens, WIDE), BF16),
        in_specs=[pl.BlockSpec(memory_space=pltpu.VMEM)] * 3,
        out_specs=pl.BlockSpec(memory_space=pltpu.VMEM),
        scratch_shapes=[
            pltpu.VMEM((HEADS, tokens // LANES, HD, LANES), F32),
            pltpu.VMEM((HEADS, tokens // LANES, HD + HALF, LANES), F32),
            pltpu.VMEM((HEADS, BLOCKS * WIDE, tokens), BF16),
            pltpu.VMEM((blocks, WIDE, WIDE), BF16),
            pltpu.VMEM((plane, units, rows, WIDE), BF16),
            pltpu.VMEM((units, rows, WIDE), BF16),
            pltpu.VMEM((max(outer, 1), units, rows, WIDE), BF16),
            pltpu.VMEM((inner, units, rows, WIDE), BF16),
            pltpu.VMEM((blocks, WIDE, WIDE), BF16),
            pltpu.VMEM((WIDE, tokens), F32),
            sems((n, plane)), sems((n, plane)),
            sems((n, max(outer, 1))), sems((n, max(outer, 1))),
            sems((n, plane)), sems((n, plane)),
        ],
        compiler_params=pltpu.CompilerParams(
            collective_id=0, has_side_effects=True, vmem_limit_bytes=60 * 1024 * 1024),
    )(queries, keys, values)


def solution(mesh):
    placed = P(("chain", "tok"), None)
    return jax.shard_map(
        functools.partial(on_device, mesh.shape["chain"], mesh.shape["tok"]),
        mesh=mesh, in_specs=(placed,) * 3, out_specs=placed, check_vma=False)
```

```python
import functools
import math

import jax
import jax.numpy as jnp
from jax import lax
from jax.experimental import pallas as pl
from jax.experimental.pallas import tpu as pltpu
from jax.sharding import PartitionSpec as P

HD = 64
HEADS = 2
WIDE = HEADS * HD
HALF = HD // 2
BLOCKS = HD // 4 + 1
LANES, DEEP = 128, 256
CHUNKS = 4
MESH = pl.DeviceIdType.MESH
F32, BF16 = jnp.float32, jnp.bfloat16


def layout(n_chain, n_tok):
    inner = 1 << ((n_chain.bit_length() - 1) // 2)
    plane = inner * n_tok
    row_parts = min(8, plane)
    blk_parts = plane // row_parts
    units = -(-BLOCKS // blk_parts)
    step = 2 if blk_parts == 1 else 1
    count = min(CHUNKS, units)
    cuts = [min(units, step * -(-units * c // (count * step))) for c in range(count + 1)]
    return inner, plane, row_parts, blk_parts, units, cuts


def pairs(low, high):
    return [tuple(range(b, min(b + 2, high))) for b in range(low, high, 2)]


def kernel(n_chain, n_tok, q_hbm, k_hbm, v_hbm, o_ref, q_ref, k_ref, v_ref, xs, zs, qf, tot, got,
           plane_sum, far_got, inc_send, inc, out_t, in_sem, rs_send, rs_recv, z_send, z_recv,
           ag_send, ag_recv):
    inner, plane, row_parts, blk_parts, units, cuts = layout(n_chain, n_tok)
    outer = n_chain // inner
    rows = WIDE // row_parts
    tokens = q_ref.shape[0]
    tiles = tokens // LANES
    chain, tok = lax.axis_index("chain"), lax.axis_index("tok")
    z, me = chain // inner, (chain % inner) * n_tok + tok

    loads = [pltpu.make_async_copy(src, dst, in_sem.at[i]) for i, (src, dst) in
             enumerate(((k_hbm, k_ref), (v_hbm, v_ref), (q_hbm, q_ref)))]
    for load in loads:
        load.start()

    def in_plane(k):
        peer = (me + k) % plane
        return peer, (z * inner + peer // n_tok, peer % n_tok)

    def along(k):
        return (((z + k) % outer) * inner + chain % inner, tok)

    barrier = pltpu.get_barrier_semaphore()
    for k in range(1, outer):
        pl.semaphore_signal(barrier, inc=1, device_id=along(k), device_id_type=MESH)
    for k in range(1, plane):
        pl.semaphore_signal(barrier, inc=1, device_id=in_plane(k)[1], device_id_type=MESH)

    root2 = math.sqrt(2.0)

    def prepare(ref):
        @pl.loop(0, tiles, unroll=4)
        def _(t):
            x = ref[pl.ds(pl.multiple_of(t * LANES, LANES), LANES), :].astype(F32).T
            for h in range(HEADS):
                own = x[h * HD:(h + 1) * HD]
                xs[h, t] = own
                wide = own * root2
                zs[h, t, pl.ds(0, HD), :] = wide
                zs[h, t, pl.ds(HD, HALF), :] = wide[:HALF]

    def feats(h, t, d):
        x = xs[h, t]
        if d == 0:
            other = x
        elif d == HALF:
            other = jnp.concatenate([x[HALF:], x[:HALF]], axis=0)
        else:
            other = zs[h, t, pl.ds(d, HD), :]
        return (x * other).astype(BF16)

    def joined(parts, axis=1):
        return parts[0] if len(parts) == 1 else jnp.concatenate(parts, axis=axis)

    def dists(b):
        return [d for d in (2 * b, 2 * b + 1) if d <= HALF]

    def blocks_of(c):
        return cuts[c] * blk_parts, cuts[c + 1] * blk_parts

    def state(c):
        low, high = blocks_of(c)
        real = min(high, BLOCKS)
        for group in pairs(low, real):
            ds = [d for b in group for d in dists(b)]
            parts = []
            for h in range(HEADS):
                part = None
                for k in range(tokens // DEEP):
                    lhs = joined([joined([feats(h, t, d) for d in ds], axis=0)
                                  for t in range(k * DEEP // LANES, (k + 1) * DEEP // LANES)])
                    more = jnp.dot(lhs, v_ref[pl.ds(k * DEEP, DEEP), :], preferred_element_type=F32)
                    part = more if part is None else part + more
                parts.append(part)
            left = lax.broadcasted_iota(jnp.int32, parts[0].shape, 1) < HD
            both = jnp.where(left, parts[0], parts[1])
            short = len(group) * WIDE - both.shape[0]
            if short:
                both = jnp.concatenate([both, jnp.zeros((short, WIDE), F32)], axis=0)
            for i, b in enumerate(group):
                tot[b] = both[i * WIDE:(i + 1) * WIDE].T.astype(BF16)
        if high > max(low, real):
            first = max(low, real)
            tot[pl.ds(first, high - first)] = jnp.zeros((high - first, WIDE, WIDE), BF16)

    def spot(c, who):
        low, _ = blocks_of(c)
        size = cuts[c + 1] - cuts[c]
        row = pl.multiple_of((who % row_parts) * rows, rows)
        return pl.ds(low + (who // row_parts) * size, size), pl.ds(row, rows)

    def span(c):
        return pl.ds(cuts[c], cuts[c + 1] - cuts[c])

    def scatter(c):
        for k in range(1, plane):
            peer, device = in_plane(k)
            blk, row = spot(c, peer)
            copy = pltpu.make_async_remote_copy(
                src_ref=tot.at[blk, row, :], dst_ref=got.at[k, span(c)],
                send_sem=rs_send.at[c, k], recv_sem=rs_recv.at[c, k],
                device_id=device, device_id_type=MESH)
            copy.start()
            rs_copies[c].append(copy)
        blk, row = spot(c, me)
        got[0, span(c)] = tot[blk, row, :]

    def piece(c, source):
        return got[(me + plane - source) % plane, span(c)].astype(F32)

    def spread(c):
        for copy in rs_copies[c]:
            copy.wait_recv()
        total = piece(c, 0)
        for source in range(1, plane):
            total = total + piece(c, source)
        plane_sum[span(c)] = total.astype(BF16)
        for k in range(1, outer):
            copy = pltpu.make_async_remote_copy(
                src_ref=plane_sum.at[span(c)], dst_ref=far_got.at[k, span(c)],
                send_sem=z_send.at[c, k], recv_sem=z_recv.at[c, k],
                device_id=along(k), device_id_type=MESH)
            copy.start()
            z_copies[c].append(copy)

    def gather(c):
        running = jnp.zeros((cuts[c + 1] - cuts[c], rows, WIDE), F32)
        for k in range(1, outer):
            z_copies[c][k - 1].wait_recv()
            running = running + jnp.where(k <= z, far_got[k, span(c)].astype(F32), 0.0)
        for g in range(inner):
            for y in range(n_tok):
                running = running + piece(c, g * n_tok + y)
            inc_send[g, span(c)] = running.astype(BF16)
        blk, row = spot(c, me)
        for k in range(1, plane):
            peer, device = in_plane(k)
            copy = pltpu.make_async_remote_copy(
                src_ref=inc_send.at[peer // n_tok, span(c)], dst_ref=inc.at[blk, row, :],
                send_sem=ag_send.at[c, k], recv_sem=ag_recv.at[c, k],
                device_id=device, device_id_type=MESH)
            copy.start()
            ag_copies[c].append(copy)
        inc[blk, row, :] = inc_send[chain % inner, span(c)]

    def expand_queries(c):
        low, high = blocks_of(c)

        @pl.loop(0, tiles)
        def _(t):
            for b in range(low, min(high, BLOCKS)):
                for d in dists(b):
                    for h in range(HEADS):
                        qf[h, t, pl.ds(d * HD, HD), :] = feats(h, t, d)

    def read(c, first, last):
        for copy in ag_copies[c]:
            copy.wait_recv()
        low, high = blocks_of(c)
        groups = pairs(low, min(high, BLOCKS))
        count = (chain + 1).astype(F32) * (tokens * n_tok)
        factor = 1.0 / (HD * jnp.sqrt(jnp.full((LANES, WIDE), count, F32)))
        for k in range(tokens // DEEP):
            at = pl.ds(k * DEEP, DEEP)
            sums = []
            for h in range(HEADS):
                row = pl.ds(h * HD, HD)
                part = None if first else out_t[row, at]
                for group in groups:
                    depth = sum(len(dists(b)) for b in group) * HD
                    state_t = joined([inc[b, row, :] for b in group])[:, :depth]
                    rhs = joined([qf[h, t, pl.ds(group[0] * WIDE, depth), :]
                                  for t in range(k * DEEP // LANES, (k + 1) * DEEP // LANES)])
                    more = jnp.dot(state_t, rhs, preferred_element_type=F32)
                    part = more if part is None else part + more
                if last:
                    sums.append(part)
                else:
                    out_t[row, at] = part
            if last:
                whole = jnp.concatenate(sums, axis=0)
                for i in range(DEEP // LANES):
                    o_ref[pl.ds(k * DEEP + i * LANES, LANES), :] = (
                        whole[:, i * LANES:(i + 1) * LANES].T * factor)

    n = len(cuts) - 1
    rs_copies, z_copies, ag_copies = ([[] for _ in range(n)] for _ in range(3))

    loads[0].wait()
    prepare(k_ref)
    loads[1].wait()
    for c in range(n):
        state(c)
        if c == 0:
            pl.semaphore_wait(barrier, plane - 1 + outer - 1)
        scatter(c)
    loads[2].wait()
    prepare(q_ref)
    for c in range(n):
        spread(c)
        expand_queries(c)
        if c == n - 1:
            for e in range(n):
                gather(e)
    for c in range(n - 1):
        read(c, c == 0, False)
    for copies in rs_copies + z_copies + ag_copies[:-1]:
        for copy in copies:
            copy.wait_send()
    read(n - 1, n == 1, True)
    for copy in ag_copies[-1]:
        copy.wait_send()


def on_device(n_chain, n_tok, queries, keys, values):
    inner, plane, row_parts, blk_parts, units, cuts = layout(n_chain, n_tok)
    outer, n = n_chain // inner, len(cuts) - 1
    rows, tokens = WIDE // row_parts, queries.shape[0]
    blocks = units * blk_parts
    sems = pltpu.SemaphoreType.DMA
    out = pl.pallas_call(
        functools.partial(kernel, n_chain, n_tok),
        out_shape=pltpu.VMEM((tokens, WIDE), F32),
        in_specs=[pl.BlockSpec(memory_space=pl.ANY)] * 3,
        out_specs=pl.BlockSpec(memory_space=pltpu.VMEM),
        scratch_shapes=[
            pltpu.VMEM((tokens, WIDE), BF16),
            pltpu.VMEM((tokens, WIDE), BF16),
            pltpu.VMEM((tokens, WIDE), BF16),
            pltpu.VMEM((HEADS, tokens // LANES, HD, LANES), F32),
            pltpu.VMEM((HEADS, tokens // LANES, HD + HALF, LANES), F32),
            pltpu.VMEM((HEADS, tokens // LANES, BLOCKS * WIDE, LANES), BF16),
            pltpu.VMEM((blocks, WIDE, WIDE), BF16),
            pltpu.VMEM((plane, units, rows, WIDE), BF16),
            pltpu.VMEM((units, rows, WIDE), BF16),
            pltpu.VMEM((max(outer, 1), units, rows, WIDE), BF16),
            pltpu.VMEM((inner, units, rows, WIDE), BF16),
            pltpu.VMEM((blocks, WIDE, WIDE), BF16),
            pltpu.VMEM((WIDE, tokens), F32),
            sems((3,)),
            sems((n, plane)), sems((n, plane)),
            sems((n, max(outer, 1))), sems((n, max(outer, 1))),
            sems((n, plane)), sems((n, plane)),
        ],
        compiler_params=pltpu.CompilerParams(
            collective_id=0, has_side_effects=True, vmem_limit_bytes=56 * 1024 * 1024),
    )(queries, keys, values)
    return out.astype(BF16)


def solution(mesh):
    placed = P(("chain", "tok"), None)
    return jax.shard_map(
        functools.partial(on_device, mesh.shape["chain"], mesh.shape["tok"]),
        mesh=mesh, in_specs=(placed,) * 3, out_specs=placed, check_vma=False)
```

```python
import functools
import math

import jax
import jax.numpy as jnp
from jax import lax
from jax.experimental import pallas as pl
from jax.experimental.pallas import tpu as pltpu
from jax.sharding import PartitionSpec as P

HD = 64
HEADS = 2
WIDE = HEADS * HD
HALF = HD // 2
BLOCKS = HD // 4 + 1
LANES, DEEP = 128, 256
CHUNKS = 9
LAG_RELAY, LAG_SUM, LAG_READ, EARLY = 3, 4, 7, 3
MESH = pl.DeviceIdType.MESH
F32, BF16 = jnp.float32, jnp.bfloat16


def layout(n_chain, n_tok):
    inner = 1 << ((n_chain.bit_length() - 1) // 2)
    plane = inner * n_tok
    row_parts = min(8, plane)
    blk_parts = plane // row_parts
    units = -(-BLOCKS // blk_parts)
    step = 2 if blk_parts == 1 else 1
    count = min(CHUNKS, units)
    cuts = [min(units, step * -(-units * c // (count * step))) for c in range(count + 1)]
    return inner, plane, row_parts, blk_parts, units, cuts


def pairs(low, high):
    return [tuple(range(b, min(b + 2, high))) for b in range(low, high, 2)]


def kernel(n_chain, n_tok, q_hbm, k_hbm, v_hbm, o_ref, q_ref, k_ref, v_ref, xs, zs, qf, tot, got,
           plane_sum, below, z_out, far_got, inc_send, inc, out_t, in_sem, rs_send, rs_recv, z_send, z_recv,
           ag_send, ag_recv):
    inner, plane, row_parts, blk_parts, units, cuts = layout(n_chain, n_tok)
    outer = n_chain // inner
    rows = WIDE // row_parts
    tokens = q_ref.shape[0]
    tiles = tokens // LANES
    chain, tok = lax.axis_index("chain"), lax.axis_index("tok")
    z, me = chain // inner, (chain % inner) * n_tok + tok
    bits = [1 << i for i in range(plane.bit_length() - 1)] if plane & (plane - 1) == 0 else []

    loads = [pltpu.make_async_copy(src, dst, in_sem.at[i]) for i, (src, dst) in
             enumerate(((k_hbm, k_ref), (v_hbm, v_ref), (q_hbm, q_ref)))]
    for load in loads:
        load.start()

    def other(k):
        return (me + k - 2 * sum(me // p % 2 * p for p in bits if k & p)) if bits else (me + k) % plane

    def in_plane(k):
        peer = other(k)
        return peer, (z * inner + peer // n_tok, peer % n_tok)

    def along(target):
        return (target * inner + chain % inner, tok)

    steps = (outer - 1).bit_length()

    def takes(s):
        return z // (1 << s) % 2 == 1

    def gives(s):
        return z % (2 << s) == (1 << s) - 1

    barrier = pltpu.get_barrier_semaphore()
    greeted = plane - 1
    for s in range(steps):
        greeted = greeted + jnp.where(gives(s), 1 << s, 0)

        @pl.when(takes(s))
        def _():
            pl.semaphore_signal(barrier, inc=1, device_id=along(z // (2 << s) * (2 << s) + (1 << s) - 1),
                                device_id_type=MESH)

    for k in range(1, plane):
        pl.semaphore_signal(barrier, inc=1, device_id=in_plane(k)[1], device_id_type=MESH)

    root2 = math.sqrt(2.0)

    def prepare(ref):
        @pl.loop(0, tiles, unroll=4)
        def _(t):
            x = ref[pl.ds(pl.multiple_of(t * LANES, LANES), LANES), :].astype(F32).T
            for h in range(HEADS):
                own = x[h * HD:(h + 1) * HD]
                xs[h, t] = own
                wide = own * root2
                zs[h, t, pl.ds(0, HD), :] = wide
                zs[h, t, pl.ds(HD, HALF), :] = wide[:HALF]

    def feats(h, t, d):
        x = xs[h, t]
        if d == 0:
            other = x
        elif d == HALF:
            other = jnp.concatenate([x[HALF:], x[:HALF]], axis=0)
        else:
            other = zs[h, t, pl.ds(d, HD), :]
        return (x * other).astype(BF16)

    def joined(parts, axis=1):
        return parts[0] if len(parts) == 1 else jnp.concatenate(parts, axis=axis)

    def dists(b):
        return [d for d in (2 * b, 2 * b + 1) if d <= HALF]

    def blocks_of(c):
        return cuts[c] * blk_parts, cuts[c + 1] * blk_parts

    def state(c):
        low, high = blocks_of(c)
        real = min(high, BLOCKS)
        for group in pairs(low, real):
            ds = [d for b in group for d in dists(b)]
            parts = []
            for h in range(HEADS):
                part = None
                for k in range(tokens // DEEP):
                    lhs = joined([joined([feats(h, t, d) for d in ds], axis=0)
                                  for t in range(k * DEEP // LANES, (k + 1) * DEEP // LANES)])
                    more = jnp.dot(lhs, v_ref[pl.ds(k * DEEP, DEEP), :], preferred_element_type=F32)
                    part = more if part is None else part + more
                parts.append(part)
            left = lax.broadcasted_iota(jnp.int32, parts[0].shape, 1) < HD
            both = jnp.where(left, parts[0], parts[1])
            short = len(group) * WIDE - both.shape[0]
            if short:
                both = jnp.concatenate([both, jnp.zeros((short, WIDE), F32)], axis=0)
            for i, b in enumerate(group):
                turned = both[i * WIDE:(i + 1) * WIDE].T.astype(BF16)
                for r in range(row_parts):
                    tot[r, b] = turned[r * rows:(r + 1) * rows]
        if high > max(low, real):
            first = max(low, real)
            tot[:, pl.ds(first, high - first)] = jnp.zeros((row_parts, high - first, rows, WIDE), BF16)

    def settle(ref, count, c, sem):
        if count > 1:
            some = ref.at[pl.ds(1, count - 1), span(c)]
            pltpu.make_async_copy(some, some, sem.at[c]).wait()

    def spot(c, who):
        low, _ = blocks_of(c)
        size = cuts[c + 1] - cuts[c]
        return who % row_parts, pl.ds(low + (who // row_parts) * size, size)

    def span(c):
        return pl.ds(cuts[c], cuts[c + 1] - cuts[c])

    def scatter(c):
        for k in range(1, plane):
            peer, device = in_plane(k)
            part, blk = spot(c, peer)
            copy = pltpu.make_async_remote_copy(
                src_ref=tot.at[part, blk], dst_ref=got.at[k, span(c)],
                send_sem=rs_send.at[c], recv_sem=rs_recv.at[c],
                device_id=device, device_id_type=MESH)
            copy.start()
        part, blk = spot(c, me)
        got[0, span(c)] = tot[part, blk]

    def piece(c, source):
        slot = other(source) if bits else (me + plane - source) % plane
        return got[slot, span(c)].astype(F32)

    def spread(c):
        settle(got, plane, c, rs_recv)
        total = piece(c, 0)
        for source in range(1, plane):
            total = total + piece(c, source)
        plane_sum[span(c)] = total
        below[span(c)] = jnp.zeros((cuts[c + 1] - cuts[c], rows, WIDE), F32)
        if steps:
            give(c, 0)

    def give(c, s):
        @pl.when(gives(s))
        def _():
            z_out[s, span(c)] = (plane_sum[span(c)] + below[span(c)]).astype(BF16)
            for k in range(1, (1 << s) + 1):
                pltpu.make_async_remote_copy(
                    src_ref=z_out.at[s, span(c)], dst_ref=far_got.at[s, span(c)],
                    send_sem=z_send.at[s, c], recv_sem=z_recv.at[s, c],
                    device_id=along(z + k), device_id_type=MESH).start()

    def take(c, s):
        @pl.when(takes(s))
        def _():
            some = far_got.at[s, span(c)]
            pltpu.make_async_copy(some, some, z_recv.at[s, c]).wait()
            below[span(c)] = below[span(c)] + far_got[s, span(c)].astype(F32)

    def relay(c, s):
        take(c, s - 1)
        give(c, s)

    def given(c, s):
        @pl.when(gives(s))
        def _():
            some = got.at[pl.ds(0, 1 << s), span(c)]
            pltpu.make_async_copy(some, some, z_send.at[s, c]).wait()

    def gather(c):
        if steps:
            take(c, steps - 1)
        running = below[span(c)]
        for g in range(inner):
            for y in range(n_tok):
                running = running + piece(c, g * n_tok + y)
            inc_send[g, span(c)] = running.astype(BF16)
        part, blk = spot(c, me)
        for k in range(1, plane):
            peer, device = in_plane(k)
            copy = pltpu.make_async_remote_copy(
                src_ref=inc_send.at[peer // n_tok, span(c)], dst_ref=inc.at[part, blk],
                send_sem=ag_send.at[c], recv_sem=ag_recv.at[c],
                device_id=device, device_id_type=MESH)
            copy.start()
        inc[part, blk] = inc_send[chain % inner, span(c)]

    def expand_queries(c):
        low, high = blocks_of(c)

        @pl.loop(0, tiles)
        def _(t):
            for b in range(low, min(high, BLOCKS)):
                for d in dists(b):
                    for h in range(HEADS):
                        qf[h, t, pl.ds(d * HD, HD), :] = feats(h, t, d)

    def read(c, first, last):
        settle(got, plane, c, ag_recv)
        low, high = blocks_of(c)
        groups = pairs(low, min(high, BLOCKS))
        count = (chain + 1).astype(F32) * (tokens * n_tok)
        factor = 1.0 / (HD * jnp.sqrt(jnp.full((LANES, WIDE), count, F32)))
        for k in range(tokens // DEEP):
            at = pl.ds(k * DEEP, DEEP)
            sums = []
            for h in range(HEADS):
                row = pl.ds(h * HD, HD)
                part = None if first else out_t[row, at]
                for group in groups:
                    depth = sum(len(dists(b)) for b in group) * HD
                    state_t = joined([joined([inc[r, b] for r in range(h * HD // rows, (h + 1) * HD // rows)],
                                             axis=0) for b in group])[:, :depth]
                    rhs = joined([qf[h, t, pl.ds(group[0] * WIDE, depth), :]
                                  for t in range(k * DEEP // LANES, (k + 1) * DEEP // LANES)])
                    more = jnp.dot(state_t, rhs, preferred_element_type=F32)
                    part = more if part is None else part + more
                if last:
                    sums.append(part)
                else:
                    out_t[row, at] = part
            if last:
                whole = jnp.concatenate(sums, axis=0)
                for i in range(DEEP // LANES):
                    o_ref[pl.ds(k * DEEP + i * LANES, LANES), :] = (
                        whole[:, i * LANES:(i + 1) * LANES].T * factor)

    n = len(cuts) - 1
    early = min(EARLY, n - 1)
    loads[0].wait()
    prepare(k_ref)
    loads[1].wait()
    for c in range(n):
        state(c)
        if c == early:
            pl.semaphore_wait(barrier, greeted)
            for e in range(c):
                scatter(e)
        if c >= early:
            scatter(c)
    loads[2].wait()
    prepare(q_ref)
    summed = LAG_RELAY * max(steps - 1, 0) + LAG_SUM
    for c in range(n + summed + LAG_READ):
        if c < n:
            spread(c)
            expand_queries(c)
        for s in range(1, steps):
            if 0 <= c - LAG_RELAY * s < n:
                relay(c - LAG_RELAY * s, s)
        if 0 <= c - summed < n:
            gather(c - summed)
        done = c - summed - LAG_READ
        if done == n - 1:
            for i in range(n):
                settle(got, plane, i, rs_send)
                for s in range(steps):
                    given(i, s)
                settle(got, plane, i, ag_send)
        if 0 <= done < n:
            read(done, done == 0, done == n - 1)


def on_device(n_chain, n_tok, queries, keys, values):
    inner, plane, row_parts, blk_parts, units, cuts = layout(n_chain, n_tok)
    outer, n = n_chain // inner, len(cuts) - 1
    rows, tokens = WIDE // row_parts, queries.shape[0]
    blocks, steps = units * blk_parts, max((outer - 1).bit_length(), 1)
    sems = pltpu.SemaphoreType.DMA
    out = pl.pallas_call(
        functools.partial(kernel, n_chain, n_tok),
        out_shape=pltpu.VMEM((tokens, WIDE), F32),
        in_specs=[pl.BlockSpec(memory_space=pl.ANY)] * 3,
        out_specs=pl.BlockSpec(memory_space=pltpu.VMEM),
        scratch_shapes=[
            pltpu.VMEM((tokens, WIDE), BF16),
            pltpu.VMEM((tokens, WIDE), BF16),
            pltpu.VMEM((tokens, WIDE), BF16),
            pltpu.VMEM((HEADS, tokens // LANES, HD, LANES), F32),
            pltpu.VMEM((HEADS, tokens // LANES, HD + HALF, LANES), F32),
            pltpu.VMEM((HEADS, tokens // LANES, BLOCKS * WIDE, LANES), BF16),
            pltpu.VMEM((row_parts, blocks, rows, WIDE), BF16),
            pltpu.VMEM((plane, units, rows, WIDE), BF16),
            pltpu.VMEM((units, rows, WIDE), F32),
            pltpu.VMEM((units, rows, WIDE), F32),
            pltpu.VMEM((steps, units, rows, WIDE), BF16),
            pltpu.VMEM((steps, units, rows, WIDE), BF16),
            pltpu.VMEM((inner, units, rows, WIDE), BF16),
            pltpu.VMEM((row_parts, blocks, rows, WIDE), BF16),
            pltpu.VMEM((WIDE, tokens), F32),
            sems((3,)),
            sems((n,)), sems((n,)), sems((steps, n)), sems((steps, n)), sems((n,)), sems((n,)),
        ],
        compiler_params=pltpu.CompilerParams(
            collective_id=0, has_side_effects=True, vmem_limit_bytes=56 * 1024 * 1024),
    )(queries, keys, values)
    return out.astype(BF16)


def solution(mesh):
    placed = P(("chain", "tok"), None)
    return jax.shard_map(
        functools.partial(on_device, mesh.shape["chain"], mesh.shape["tok"]),
        mesh=mesh, in_specs=(placed,) * 3, out_specs=placed, check_vma=False)
```

```python
import functools
import math

import jax
import jax.numpy as jnp
from jax import lax
from jax.experimental import pallas as pl
from jax.experimental.pallas import tpu as pltpu
from jax.sharding import PartitionSpec as P

HD = 64
HEADS = 2
WIDE = HEADS * HD
HALF = HD // 2
BLOCKS = HD // 4 + 1
LANES, DEEP = 128, 256
CHUNKS = 9
LAG_RELAY, LAG_SUM, LAG_READ, EARLY = 2, 4, 7, 3
MESH = pl.DeviceIdType.MESH
F32, BF16 = jnp.float32, jnp.bfloat16


def layout(n_chain, n_tok):
    inner = 1 << ((n_chain.bit_length() - 1) // 2)
    plane = inner * n_tok
    row_parts = min(8, plane)
    blk_parts = plane // row_parts
    units = -(-BLOCKS // blk_parts)
    step = 2 if blk_parts == 1 else 1
    count = min(CHUNKS, units)
    cuts = [min(units, step * -(-units * c // (count * step))) for c in range(count + 1)]
    return inner, plane, row_parts, blk_parts, units, cuts


def pairs(low, high):
    return [tuple(range(b, min(b + 2, high))) for b in range(low, high, 2)]


def kernel(n_chain, n_tok, q_hbm, k_hbm, v_hbm, o_ref, q_ref, k_ref, v_ref, xs, zs, qf, tot, got,
           plane_sum, below, z_out, far_got, inc_send, inc, out_t, in_sem, rs_send, rs_recv, z_send, z_recv,
           ag_send, ag_recv):
    inner, plane, row_parts, blk_parts, units, cuts = layout(n_chain, n_tok)
    outer = n_chain // inner
    rows = WIDE // row_parts
    tokens = q_ref.shape[0]
    tiles = tokens // LANES
    chain, tok = lax.axis_index("chain"), lax.axis_index("tok")
    z, me = chain // inner, (chain % inner) * n_tok + tok
    bits = [1 << i for i in range(plane.bit_length() - 1)] if plane & (plane - 1) == 0 else []

    loads = [pltpu.make_async_copy(src, dst, in_sem.at[i]) for i, (src, dst) in
             enumerate(((k_hbm, k_ref), (v_hbm, v_ref), (q_hbm, q_ref)))]
    for load in loads:
        load.start()

    def other(k):
        return (me + k - 2 * sum(me // p % 2 * p for p in bits if k & p)) if bits else (me + k) % plane

    def in_plane(k):
        peer = other(k)
        return peer, (z * inner + peer // n_tok, peer % n_tok)

    def along(target):
        return (target * inner + chain % inner, tok)

    steps = (outer - 1).bit_length()

    def takes(s):
        return z // (1 << s) % 2 == 1

    def gives(s):
        return z % (2 << s) == (1 << s) - 1

    barrier = pltpu.get_barrier_semaphore()
    greeted = plane - 1
    for s in range(steps):
        greeted = greeted + jnp.where(gives(s), 1 << s, 0)

        @pl.when(takes(s))
        def _():
            pl.semaphore_signal(barrier, inc=1, device_id=along(z // (2 << s) * (2 << s) + (1 << s) - 1),
                                device_id_type=MESH)

    for k in range(1, plane):
        pl.semaphore_signal(barrier, inc=1, device_id=in_plane(k)[1], device_id_type=MESH)

    root2 = math.sqrt(2.0)

    def prepare(ref):
        @pl.loop(0, tiles, unroll=4)
        def _(t):
            x = ref[pl.ds(pl.multiple_of(t * LANES, LANES), LANES), :].astype(F32).T
            for h in range(HEADS):
                own = x[h * HD:(h + 1) * HD]
                xs[h, t] = own
                wide = own * root2
                zs[h, t, pl.ds(0, HD), :] = wide
                zs[h, t, pl.ds(HD, HALF), :] = wide[:HALF]

    def feats(h, t, d):
        x = xs[h, t]
        if d == 0:
            other = x
        elif d == HALF:
            other = jnp.concatenate([x[HALF:], x[:HALF]], axis=0)
        else:
            other = zs[h, t, pl.ds(d, HD), :]
        return (x * other).astype(BF16)

    def joined(parts, axis=1):
        return parts[0] if len(parts) == 1 else jnp.concatenate(parts, axis=axis)

    def dists(b):
        return [d for d in (2 * b, 2 * b + 1) if d <= HALF]

    def blocks_of(c):
        return cuts[c] * blk_parts, cuts[c + 1] * blk_parts

    def state(c):
        low, high = blocks_of(c)
        real = min(high, BLOCKS)
        for group in pairs(low, real):
            ds = [d for b in group for d in dists(b)]
            parts = []
            for h in range(HEADS):
                part = None
                for k in range(tokens // DEEP):
                    lhs = joined([joined([feats(h, t, d) for d in ds], axis=0)
                                  for t in range(k * DEEP // LANES, (k + 1) * DEEP // LANES)])
                    more = jnp.dot(lhs, v_ref[pl.ds(k * DEEP, DEEP), :], preferred_element_type=F32)
                    part = more if part is None else part + more
                parts.append(part)
            left = lax.broadcasted_iota(jnp.int32, parts[0].shape, 1) < HD
            both = jnp.where(left, parts[0], parts[1])
            short = len(group) * WIDE - both.shape[0]
            if short:
                both = jnp.concatenate([both, jnp.zeros((short, WIDE), F32)], axis=0)
            for i, b in enumerate(group):
                turned = both[i * WIDE:(i + 1) * WIDE].T.astype(BF16)
                for r in range(row_parts):
                    tot[r, b] = turned[r * rows:(r + 1) * rows]
        if high > max(low, real):
            first = max(low, real)
            tot[:, pl.ds(first, high - first)] = jnp.zeros((row_parts, high - first, rows, WIDE), BF16)

    def settle(ref, count, c, sem):
        if count > 1:
            some = ref.at[pl.ds(1, count - 1), span(c)]
            pltpu.make_async_copy(some, some, sem.at[c]).wait()

    def spot(c, who):
        low, _ = blocks_of(c)
        size = cuts[c + 1] - cuts[c]
        return who % row_parts, pl.ds(low + (who // row_parts) * size, size)

    def span(c):
        return pl.ds(cuts[c], cuts[c + 1] - cuts[c])

    def scatter(c):
        for k in range(1, plane):
            peer, device = in_plane(k)
            part, blk = spot(c, peer)
            copy = pltpu.make_async_remote_copy(
                src_ref=tot.at[part, blk], dst_ref=got.at[k, span(c)],
                send_sem=rs_send.at[c], recv_sem=rs_recv.at[c],
                device_id=device, device_id_type=MESH)
            copy.start()
        part, blk = spot(c, me)
        got[0, span(c)] = tot[part, blk]

    def piece(c, source):
        slot = other(source) if bits else (me + plane - source) % plane
        return got[slot, span(c)].astype(F32)

    def spread(c):
        settle(got, plane, c, rs_recv)
        total = piece(c, 0)
        for source in range(1, plane):
            total = total + piece(c, source)
        plane_sum[span(c)] = total
        below[span(c)] = jnp.zeros((cuts[c + 1] - cuts[c], rows, WIDE), F32)
        if steps:
            give(c, 0)

    def give(c, s):
        @pl.when(gives(s))
        def _():
            z_out[s, span(c)] = (plane_sum[span(c)] + below[span(c)]).astype(BF16)
            for k in range(1, (1 << s) + 1):
                pltpu.make_async_remote_copy(
                    src_ref=z_out.at[s, span(c)], dst_ref=far_got.at[s, span(c)],
                    send_sem=z_send.at[s, c], recv_sem=z_recv.at[s, c],
                    device_id=along(z + k), device_id_type=MESH).start()

    def take(c, s):
        @pl.when(takes(s))
        def _():
            some = far_got.at[s, span(c)]
            pltpu.make_async_copy(some, some, z_recv.at[s, c]).wait()
            below[span(c)] = below[span(c)] + far_got[s, span(c)].astype(F32)

    def relay(c, s):
        take(c, s - 1)
        give(c, s)

    def given(c, s):
        @pl.when(gives(s))
        def _():
            some = got.at[pl.ds(0, 1 << s), span(c)]
            pltpu.make_async_copy(some, some, z_send.at[s, c]).wait()

    def gather(c):
        if steps:
            take(c, steps - 1)
        running = below[span(c)]
        for g in range(inner):
            for y in range(n_tok):
                running = running + piece(c, g * n_tok + y)
            inc_send[g, span(c)] = running.astype(BF16)
        part, blk = spot(c, me)
        for k in range(1, plane):
            peer, device = in_plane(k)
            copy = pltpu.make_async_remote_copy(
                src_ref=inc_send.at[peer // n_tok, span(c)], dst_ref=inc.at[part, blk],
                send_sem=ag_send.at[c], recv_sem=ag_recv.at[c],
                device_id=device, device_id_type=MESH)
            copy.start()
        inc[part, blk] = inc_send[chain % inner, span(c)]

    def expand_queries(c):
        low, high = blocks_of(c)

        @pl.loop(0, tiles)
        def _(t):
            for b in range(low, min(high, BLOCKS)):
                for d in dists(b):
                    for h in range(HEADS):
                        qf[h, t, pl.ds(d * HD, HD), :] = feats(h, t, d)

    def read(c, first, last):
        settle(got, plane, c, ag_recv)
        low, high = blocks_of(c)
        groups = pairs(low, min(high, BLOCKS))
        count = (chain + 1).astype(F32) * (tokens * n_tok)
        factor = 1.0 / (HD * jnp.sqrt(jnp.full((LANES, WIDE), count, F32)))
        for k in range(tokens // DEEP):
            at = pl.ds(k * DEEP, DEEP)
            sums = []
            for h in range(HEADS):
                row = pl.ds(h * HD, HD)
                part = None if first else out_t[row, at]
                for group in groups:
                    depth = sum(len(dists(b)) for b in group) * HD
                    state_t = joined([joined([inc[r, b] for r in range(h * HD // rows, (h + 1) * HD // rows)],
                                             axis=0) for b in group])[:, :depth]
                    rhs = joined([qf[h, t, pl.ds(group[0] * WIDE, depth), :]
                                  for t in range(k * DEEP // LANES, (k + 1) * DEEP // LANES)])
                    more = jnp.dot(state_t, rhs, preferred_element_type=F32)
                    part = more if part is None else part + more
                if last:
                    sums.append(part)
                else:
                    out_t[row, at] = part
            if last:
                whole = jnp.concatenate(sums, axis=0)
                for i in range(DEEP // LANES):
                    o_ref[pl.ds(k * DEEP + i * LANES, LANES), :] = (
                        whole[:, i * LANES:(i + 1) * LANES].T * factor)

    n = len(cuts) - 1
    early = min(EARLY, n - 1)
    loads[0].wait()
    prepare(k_ref)
    loads[1].wait()
    for c in range(n):
        state(c)
        if c == early:
            pl.semaphore_wait(barrier, greeted)
            for e in range(c):
                scatter(e)
        if c >= early:
            scatter(c)
    loads[2].wait()
    prepare(q_ref)
    summed = LAG_RELAY * max(steps - 1, 0) + LAG_SUM
    for c in range(n + summed + LAG_READ):
        if c < n:
            spread(c)
            expand_queries(c)
        for s in range(1, steps):
            if 0 <= c - LAG_RELAY * s < n:
                relay(c - LAG_RELAY * s, s)
        if 0 <= c - summed < n:
            gather(c - summed)
        done = c - summed - LAG_READ
        if done == n - 1:
            for i in range(n):
                settle(got, plane, i, rs_send)
                for s in range(steps):
                    given(i, s)
                settle(got, plane, i, ag_send)
        if 0 <= done < n:
            read(done, done == 0, done == n - 1)


def on_device(n_chain, n_tok, queries, keys, values):
    inner, plane, row_parts, blk_parts, units, cuts = layout(n_chain, n_tok)
    outer, n = n_chain // inner, len(cuts) - 1
    rows, tokens = WIDE // row_parts, queries.shape[0]
    blocks, steps = units * blk_parts, max((outer - 1).bit_length(), 1)
    sems = pltpu.SemaphoreType.DMA
    out = pl.pallas_call(
        functools.partial(kernel, n_chain, n_tok),
        out_shape=pltpu.VMEM((tokens, WIDE), F32),
        in_specs=[pl.BlockSpec(memory_space=pl.ANY)] * 3,
        out_specs=pl.BlockSpec(memory_space=pltpu.VMEM),
        scratch_shapes=[
            pltpu.VMEM((tokens, WIDE), BF16),
            pltpu.VMEM((tokens, WIDE), BF16),
            pltpu.VMEM((tokens, WIDE), BF16),
            pltpu.VMEM((HEADS, tokens // LANES, HD, LANES), F32),
            pltpu.VMEM((HEADS, tokens // LANES, HD + HALF, LANES), F32),
            pltpu.VMEM((HEADS, tokens // LANES, BLOCKS * WIDE, LANES), BF16),
            pltpu.VMEM((row_parts, blocks, rows, WIDE), BF16),
            pltpu.VMEM((plane, units, rows, WIDE), BF16),
            pltpu.VMEM((units, rows, WIDE), F32),
            pltpu.VMEM((units, rows, WIDE), F32),
            pltpu.VMEM((steps, units, rows, WIDE), BF16),
            pltpu.VMEM((steps, units, rows, WIDE), BF16),
            pltpu.VMEM((inner, units, rows, WIDE), BF16),
            pltpu.VMEM((row_parts, blocks, rows, WIDE), BF16),
            pltpu.VMEM((WIDE, tokens), F32),
            sems((3,)),
            sems((n,)), sems((n,)), sems((steps, n)), sems((steps, n)), sems((n,)), sems((n,)),
        ],
        compiler_params=pltpu.CompilerParams(
            collective_id=0, has_side_effects=True, vmem_limit_bytes=56 * 1024 * 1024),
    )(queries, keys, values)
    return out.astype(BF16)


def solution(mesh):
    placed = P(("chain", "tok"), None)
    return jax.shard_map(
        functools.partial(on_device, mesh.shape["chain"], mesh.shape["tok"]),
        mesh=mesh, in_specs=(placed,) * 3, out_specs=placed, check_vma=False)
```

```python
import functools
import math

import jax
import jax.numpy as jnp
from jax import lax
from jax.experimental import pallas as pl
from jax.experimental.pallas import tpu as pltpu
from jax.sharding import PartitionSpec as P

HD = 64
HEADS = 2
WIDE = HEADS * HD
HALF = HD // 2
BLOCKS = HD // 4 + 1
LANES, DEEP = 128, 256
CHUNKS = 9
LAG_RELAY, LAG_SUM, LAG_READ, EARLY = 2, 4, 8, 3
MESH = pl.DeviceIdType.MESH
F32, BF16 = jnp.float32, jnp.bfloat16


def layout(n_chain, n_tok):
    inner = 1 << ((n_chain.bit_length() - 1) // 2)
    plane = inner * n_tok
    row_parts = min(8, plane)
    blk_parts = plane // row_parts
    units = -(-BLOCKS // blk_parts)
    step = 2 if blk_parts == 1 else 1
    count = min(CHUNKS, units)
    cuts = [min(units, step * -(-units * c // (count * step))) for c in range(count + 1)]
    if step == 2 and count > 2:
        cuts = cuts[:1] + [c - 1 for c in cuts[1:-1]] + [units - 1, units]
    return inner, plane, row_parts, blk_parts, units, cuts


def pairs(low, high):
    return [tuple(range(b, min(b + 2, high))) for b in range(low, high, 2)]


def kernel(n_chain, n_tok, q_hbm, k_hbm, v_hbm, o_ref, q_ref, k_ref, v_ref, xs, zs, qf, tot, got,
           plane_sum, below, z_out, far_got, inc_send, inc, out_t, in_sem, rs_send, rs_recv, z_send, z_recv,
           ag_send, ag_recv):
    inner, plane, row_parts, blk_parts, units, cuts = layout(n_chain, n_tok)
    outer = n_chain // inner
    rows = WIDE // row_parts
    tokens = q_ref.shape[0]
    tiles = tokens // LANES
    chain, tok = lax.axis_index("chain"), lax.axis_index("tok")
    z, me = chain // inner, (chain % inner) * n_tok + tok
    bits = [1 << i for i in range(plane.bit_length() - 1)] if plane & (plane - 1) == 0 else []

    loads = [pltpu.make_async_copy(src, dst, in_sem.at[i]) for i, (src, dst) in
             enumerate(((k_hbm, k_ref), (v_hbm, v_ref), (q_hbm, q_ref)))]
    for load in loads:
        load.start()

    def other(k):
        return (me + k - 2 * sum(me // p % 2 * p for p in bits if k & p)) if bits else (me + k) % plane

    def in_plane(k):
        peer = other(k)
        return peer, (z * inner + peer // n_tok, peer % n_tok)

    def along(target):
        return (target * inner + chain % inner, tok)

    steps = (outer - 1).bit_length()

    def takes(s):
        return z // (1 << s) % 2 == 1

    def gives(s):
        return z % (2 << s) == (1 << s) - 1

    barrier = pltpu.get_barrier_semaphore()
    for k in range(1, plane):
        pl.semaphore_signal(barrier, inc=1, device_id=in_plane(k)[1], device_id_type=MESH)
    greeted = plane - 1
    for s in range(steps):
        greeted = greeted + jnp.where(gives(s), 1 << s, 0)

        @pl.when(takes(s))
        def _():
            pl.semaphore_signal(barrier, inc=1, device_id=along(z // (2 << s) * (2 << s) + (1 << s) - 1),
                                device_id_type=MESH)

    root2 = math.sqrt(2.0)

    def prepare(ref):
        @pl.loop(0, tiles, unroll=4)
        def _(t):
            x = ref[pl.ds(pl.multiple_of(t * LANES, LANES), LANES), :].astype(F32).T
            for h in range(HEADS):
                own = x[h * HD:(h + 1) * HD]
                xs[h, t] = own
                wide = own * root2
                zs[h, t, pl.ds(0, HD), :] = wide
                zs[h, t, pl.ds(HD, HALF), :] = wide[:HALF]

    def feats(h, t, d):
        x = xs[h, t]
        if d == 0:
            other = x
        elif d == HALF:
            other = jnp.concatenate([x[HALF:], x[:HALF]], axis=0)
        else:
            other = zs[h, t, pl.ds(d, HD), :]
        return (x * other).astype(BF16)

    def joined(parts, axis=1):
        return parts[0] if len(parts) == 1 else jnp.concatenate(parts, axis=axis)

    def dists(b):
        return [d for d in (2 * b, 2 * b + 1) if d <= HALF]

    def blocks_of(c):
        return cuts[c] * blk_parts, cuts[c + 1] * blk_parts

    def state(c):
        low, high = blocks_of(c)
        real = min(high, BLOCKS)
        for group in pairs(low, real):
            ds = [d for b in group for d in dists(b)]
            parts = []
            for h in range(HEADS):
                part = None
                for k in range(tokens // DEEP):
                    lhs = joined([joined([feats(h, t, d) for d in ds], axis=0)
                                  for t in range(k * DEEP // LANES, (k + 1) * DEEP // LANES)])
                    more = jnp.dot(lhs, v_ref[pl.ds(k * DEEP, DEEP), :], preferred_element_type=F32)
                    part = more if part is None else part + more
                parts.append(part)
            left = lax.broadcasted_iota(jnp.int32, parts[0].shape, 1) < HD
            both = jnp.where(left, parts[0], parts[1])
            short = len(group) * WIDE - both.shape[0]
            if short:
                both = jnp.concatenate([both, jnp.zeros((short, WIDE), F32)], axis=0)
            for i, b in enumerate(group):
                turned = both[i * WIDE:(i + 1) * WIDE].T.astype(BF16)
                for r in range(row_parts):
                    tot[r, b] = turned[r * rows:(r + 1) * rows]
        if high > max(low, real):
            first = max(low, real)
            tot[:, pl.ds(first, high - first)] = jnp.zeros((row_parts, high - first, rows, WIDE), BF16)

    def settle(ref, count, c, sem):
        if count > 1:
            some = ref.at[pl.ds(1, count - 1), span(c)]
            pltpu.make_async_copy(some, some, sem.at[c]).wait()

    def spot(c, who):
        low, _ = blocks_of(c)
        size = cuts[c + 1] - cuts[c]
        return who % row_parts, pl.ds(low + (who // row_parts) * size, size)

    def span(c):
        return pl.ds(cuts[c], cuts[c + 1] - cuts[c])

    def scatter(c):
        for k in range(1, plane):
            peer, device = in_plane(k)
            part, blk = spot(c, peer)
            copy = pltpu.make_async_remote_copy(
                src_ref=tot.at[part, blk], dst_ref=got.at[k, span(c)],
                send_sem=rs_send.at[c], recv_sem=rs_recv.at[c],
                device_id=device, device_id_type=MESH)
            copy.start()
        part, blk = spot(c, me)
        got[0, span(c)] = tot[part, blk]

    def piece(c, source):
        slot = other(source) if bits else (me + plane - source) % plane
        return got[slot, span(c)].astype(F32)

    def spread(c):
        settle(got, plane, c, rs_recv)
        total = piece(c, 0)
        for source in range(1, plane):
            total = total + piece(c, source)
        plane_sum[span(c)] = total
        below[span(c)] = jnp.zeros((cuts[c + 1] - cuts[c], rows, WIDE), F32)
        if steps:
            give(c, 0)

    def give(c, s):
        @pl.when(gives(s))
        def _():
            z_out[s, span(c)] = (plane_sum[span(c)] + below[span(c)]).astype(BF16)
            for k in range(1, (1 << s) + 1):
                pltpu.make_async_remote_copy(
                    src_ref=z_out.at[s, span(c)], dst_ref=far_got.at[s, span(c)],
                    send_sem=z_send.at[s, c], recv_sem=z_recv.at[s, c],
                    device_id=along(z + k), device_id_type=MESH).start()

    def take(c, s):
        @pl.when(takes(s))
        def _():
            some = far_got.at[s, span(c)]
            pltpu.make_async_copy(some, some, z_recv.at[s, c]).wait()
            below[span(c)] = below[span(c)] + far_got[s, span(c)].astype(F32)

    def relay(c, s):
        take(c, s - 1)
        give(c, s)

    def given(c, s):
        @pl.when(gives(s))
        def _():
            some = got.at[pl.ds(0, 1 << s), span(c)]
            pltpu.make_async_copy(some, some, z_send.at[s, c]).wait()

    def gather(c):
        if steps:
            take(c, steps - 1)
        running = below[span(c)]
        for g in range(inner):
            for y in range(n_tok):
                running = running + piece(c, g * n_tok + y)
            inc_send[g, span(c)] = running.astype(BF16)
        part, blk = spot(c, me)
        for k in range(1, plane):
            peer, device = in_plane(k)
            copy = pltpu.make_async_remote_copy(
                src_ref=inc_send.at[peer // n_tok, span(c)], dst_ref=inc.at[part, blk],
                send_sem=ag_send.at[c], recv_sem=ag_recv.at[c],
                device_id=device, device_id_type=MESH)
            copy.start()
        inc[part, blk] = inc_send[chain % inner, span(c)]

    def expand_queries(c):
        low, high = blocks_of(c)

        @pl.loop(0, tiles)
        def _(t):
            for b in range(low, min(high, BLOCKS)):
                for d in dists(b):
                    for h in range(HEADS):
                        qf[h, t, pl.ds(d * HD, HD), :] = feats(h, t, d)

    def read(c, first, last):
        settle(got, plane, c, ag_recv)
        low, high = blocks_of(c)
        groups = pairs(low, min(high, BLOCKS))
        count = (chain + 1).astype(F32) * (tokens * n_tok)
        factor = 1.0 / (HD * jnp.sqrt(jnp.full((LANES, WIDE), count, F32)))
        for k in range(tokens // DEEP):
            at = pl.ds(k * DEEP, DEEP)
            sums = []
            for h in range(HEADS):
                row = pl.ds(h * HD, HD)
                part = None if first else out_t[row, at]
                for group in groups:
                    depth = sum(len(dists(b)) for b in group) * HD
                    state_t = joined([joined([inc[r, b] for r in range(h * HD // rows, (h + 1) * HD // rows)],
                                             axis=0) for b in group])[:, :depth]
                    rhs = joined([qf[h, t, pl.ds(group[0] * WIDE, depth), :]
                                  for t in range(k * DEEP // LANES, (k + 1) * DEEP // LANES)])
                    more = jnp.dot(state_t, rhs, preferred_element_type=F32)
                    part = more if part is None else part + more
                if last:
                    sums.append(part)
                else:
                    out_t[row, at] = part
            if last:
                whole = jnp.concatenate(sums, axis=0)
                for i in range(DEEP // LANES):
                    o_ref[pl.ds(k * DEEP + i * LANES, LANES), :] = (
                        whole[:, i * LANES:(i + 1) * LANES].T * factor).astype(BF16)

    n = len(cuts) - 1
    early = min(EARLY, n - 1)
    loads[0].wait()
    prepare(k_ref)
    loads[1].wait()
    for c in range(n):
        state(c)
        if c == early:
            pl.semaphore_wait(barrier, greeted)
            for e in range(c):
                scatter(e)
        if c >= early:
            scatter(c)
    loads[2].wait()
    summed = LAG_RELAY * max(steps - 1, 0) + LAG_SUM
    for c in range(n + summed + LAG_READ):
        if c < n:
            spread(c)
            if c == 0:
                prepare(q_ref)
            expand_queries(c)
        for s in range(1, steps):
            if 0 <= c - LAG_RELAY * s < n:
                relay(c - LAG_RELAY * s, s)
        if 0 <= c - summed < n:
            gather(c - summed)
        done = c - summed - LAG_READ
        if done == n - 1:
            for i in range(n):
                settle(got, plane, i, rs_send)
                for s in range(steps):
                    given(i, s)
                settle(got, plane, i, ag_send)
        if 0 <= done < n:
            read(done, done == 0, done == n - 1)


def on_device(n_chain, n_tok, queries, keys, values):
    inner, plane, row_parts, blk_parts, units, cuts = layout(n_chain, n_tok)
    outer, n = n_chain // inner, len(cuts) - 1
    rows, tokens = WIDE // row_parts, queries.shape[0]
    blocks, steps = units * blk_parts, max((outer - 1).bit_length(), 1)
    sems = pltpu.SemaphoreType.DMA
    out = pl.pallas_call(
        functools.partial(kernel, n_chain, n_tok),
        out_shape=pltpu.VMEM((tokens, WIDE), BF16),
        in_specs=[pl.BlockSpec(memory_space=pl.ANY)] * 3,
        out_specs=pl.BlockSpec(memory_space=pltpu.VMEM),
        scratch_shapes=[
            pltpu.VMEM((tokens, WIDE), BF16),
            pltpu.VMEM((tokens, WIDE), BF16),
            pltpu.VMEM((tokens, WIDE), BF16),
            pltpu.VMEM((HEADS, tokens // LANES, HD, LANES), F32),
            pltpu.VMEM((HEADS, tokens // LANES, HD + HALF, LANES), F32),
            pltpu.VMEM((HEADS, tokens // LANES, BLOCKS * WIDE, LANES), BF16),
            pltpu.VMEM((row_parts, blocks, rows, WIDE), BF16),
            pltpu.VMEM((plane, units, rows, WIDE), BF16),
            pltpu.VMEM((units, rows, WIDE), F32),
            pltpu.VMEM((units, rows, WIDE), F32),
            pltpu.VMEM((steps, units, rows, WIDE), BF16),
            pltpu.VMEM((steps, units, rows, WIDE), BF16),
            pltpu.VMEM((inner, units, rows, WIDE), BF16),
            pltpu.VMEM((row_parts, blocks, rows, WIDE), BF16),
            pltpu.VMEM((WIDE, tokens), F32),
            sems((3,)),
            sems((n,)), sems((n,)), sems((steps, n)), sems((steps, n)), sems((n,)), sems((n,)),
        ],
        compiler_params=pltpu.CompilerParams(
            collective_id=0, has_side_effects=True, vmem_limit_bytes=56 * 1024 * 1024),
    )(queries, keys, values)
    return out


def solution(mesh):
    placed = P(("chain", "tok"), None)
    return jax.shard_map(
        functools.partial(on_device, mesh.shape["chain"], mesh.shape["tok"]),
        mesh=mesh, in_specs=(placed,) * 3, out_specs=placed, check_vma=False)
```
